32 devices in a mesh: member: 2 (over y), seq: 4 (over z), head: 2 (over x), rep: 2 (over core).
Axes of the slice: x: 2, y: 2, z: 4, core: 2. Of those that a mesh axis runs over, the one named last changes fastest.
Arguments:
- x_raw: bfloat16 [4, 4096, 2560], P(('member', 'rep'), 'seq', 'head'), parts along dimension 0, may hold values from -6 to 6
- bc_raw: bfloat16 [4, 4096, 256], P(('member', 'rep'), 'seq'), parts along dimension 0, may hold values from -3 to 3
- gate_in: bfloat16 [4, 4096, 2560], P(('member', 'rep'), 'seq', 'head'), parts along dimension 0, may hold values from -570 to 570
- step_raw: float32 [4, 4096, 40], P(('member', 'rep'), 'seq', 'head'), parts along dimension 0, may hold values from -1.9 to 4.9
- conv_x_weight: bfloat16 [8, 2560], P('member', 'head'), parts along dimension 0, may hold values from -3 to 3
- conv_x_bias: bfloat16 [5120], P(('member', 'head')), parts along dimension 0, may hold values from -0.5 to 0.5
- conv_bc_weight: bfloat16 [8, 256], P('member'), parts along dimension 0, may hold values from -3 to 3
- conv_bc_bias: bfloat16 [512], P('member'), parts along dimension 0, may hold values from -0.5 to 0.5
- dt_bias: float32 [80], P(('member', 'head')), parts along dimension 0, may hold values from -3.5 to 0.55
- a_log: float32 [80], P(('member', 'head')), parts along dimension 0
- d_skip: float32 [80], P(('member', 'head')), parts along dimension 0, may hold values from 0.5 to 2
- norm_gain: float32 [5120], P(('member', 'head')), parts along dimension 0, may hold values from 0.5 to 1.5
Outputs:
- mixer_out: bfloat16 [4, 4096, 2560], P(('member', 'rep'), 'seq', 'head'), parts along dimension 0
The draws below stay inside these ranges and needn't reach their ends.
There are 2 independent parts, one for each index of `member`. The reference program is written for one: setup_inputs(seed, part) draws one part's arguments, and reference() takes and returns one part's arrays. A program takes and returns all parts, laid end to end along the dimension named above; each array names one. Nothing has to cross between parts.
All inputs are finite; a program needn't handle non-finite values.
Results may differ from the reference program's by a relative error of at most 0.0082.
Values may be sent and summed in bfloat16 or wider, within the bound.
A program may use at most 64 MiB of HBM per device.

```python
import math
import jax
import jax.numpy as jnp
from jax import lax

HEADS = 40
HEADDIM = 64
STATE = 128
GROUP = 256
CONV = 4
TOK_DEV = 1024
DI = 2560
LENGTH = 4096
SEQS = 2


def head_plan(key):
    slow_share = 0.5
    chooser = jax.random.uniform(jax.random.fold_in(key, 7001), (HEADS,))
    slow_heads = chooser < slow_share

    def spread_log(label, lowest, highest):
        unit_draw = jax.random.uniform(jax.random.fold_in(key, label), (HEADS,))
        return jnp.exp(math.log(lowest) + unit_draw * (math.log(highest) - math.log(lowest)))
    base_step = jnp.where(slow_heads, spread_log(7002, 0.03, 0.1), spread_log(7003, 0.3, 1.0))
    slow_rate = spread_log(7004, 0.2, 0.6) / LENGTH
    decay_rate = jnp.where(slow_heads, slow_rate, spread_log(7005, 0.02, 0.1))
    return (base_step, decay_rate / base_step)


def draw_dt_bias(key, part):
    base_step, head_rate = head_plan(key)
    return jnp.log(jnp.expm1(base_step)).astype(jnp.float32)


def draw_a_log(key, part):
    base_step, head_rate = head_plan(key)
    return jnp.log(head_rate).astype(jnp.float32)


def draw_step_raw(key, part):
    blocks = LENGTH // TOK_DEV
    offsets = jax.random.uniform(jax.random.fold_in(key, 1), (SEQS, blocks, 1, HEADS), minval=-0.7, maxval=0.7)
    offsets = jnp.broadcast_to(offsets, (SEQS, blocks, TOK_DEV, HEADS)).reshape(SEQS, LENGTH, HEADS)
    jitter = jnp.clip(0.3 * jax.random.normal(jax.random.fold_in(key, 2), (SEQS, LENGTH, HEADS)), -1.2, 1.2)
    run_length = max(LENGTH // 32, 1)
    starts = jax.random.randint(jax.random.fold_in(key, 3), (SEQS, 3), 0, LENGTH - run_length + 1)
    places = jnp.arange(LENGTH)
    inside = jnp.any((places[None, None, :] >= starts[:, :, None]) & (places[None, None, :] < starts[:, :, None] + run_length), axis=1)
    return (offsets + jitter + 3.0 * inside[:, :, None].astype(jnp.float32)).astype(jnp.float32)


def draw_gate_in(key, part):
    channel_ramp = jnp.arange(DI).astype(jnp.float32) / DI
    noise_cols = jax.random.uniform(jax.random.fold_in(key, 11), (DI,), minval=-0.35, maxval=0.35)
    noise_rows = jax.random.uniform(jax.random.fold_in(key, 12), (SEQS, LENGTH, 1))
    columns = jnp.exp(math.log(10.0) * channel_ramp + noise_cols)
    row_scale = jnp.exp(math.log(4.0) * noise_rows)
    values = jnp.clip(jax.random.normal(jax.random.fold_in(key, 13), (SEQS, LENGTH, DI)), -4.0, 4.0)
    return (values * columns * row_scale).astype(jnp.bfloat16)


def level_of(stream_key, extent, split, low, high):
    factor_of = 1.0
    for dim, shards_of in split:
        draws = jax.random.uniform(jax.random.fold_in(jax.random.fold_in(stream_key, 6), dim), (shards_of,), jnp.float32, low / len(split), high / len(split))
        factor_of = factor_of * jnp.repeat(jnp.exp(draws), extent[dim] // shards_of).reshape((-1,) + (1,) * (len(extent) - 1 - dim))
    return factor_of


def bell_draw(key, shape, deviation, limit, cuts=(), dtype=jnp.bfloat16):
    drawn = jax.random.normal(key, shape, jnp.float32) * deviation
    if len(cuts) > 0:
        drawn = level_of(key, shape, cuts, -0.22, 0.18) * drawn
    return jnp.clip(drawn, min=-limit, max=limit).astype(dtype)


def setup_inputs(seed: int = 0, part: int = 0) -> dict:
    arg_keys = jax.random.split(jax.random.key(seed), 13)
    own_keys = jax.random.split(jax.random.fold_in(arg_keys[12], part), 13)
    return {
        "x_raw": bell_draw(own_keys[0], (SEQS, LENGTH, DI), 1.0, 6.0, ((0, 2), (1, 4), (2, 2))),
        "bc_raw": bell_draw(own_keys[1], (SEQS, LENGTH, 2 * STATE), 0.5, 3.0, ((0, 2), (1, 4))),
        "gate_in": draw_gate_in(jax.random.fold_in(jax.random.fold_in(arg_keys[12], part), 71), part),
        "step_raw": draw_step_raw(jax.random.fold_in(jax.random.fold_in(arg_keys[12], part), 71), part),
        "conv_x_weight": bell_draw(own_keys[4], (CONV, DI), CONV ** -0.5, 3.0, ((1, 2),)),
        "conv_x_bias": jnp.clip(jax.random.uniform(own_keys[5], (DI,), jnp.float32, -0.5, 0.5) * level_of(own_keys[5], (DI,), ((0, 2),), -0.4, 0.0), -0.5, 0.5).astype(jnp.bfloat16),
        "conv_bc_weight": bell_draw(own_keys[6], (CONV, 2 * STATE), CONV ** -0.5, 3.0),
        "conv_bc_bias": jnp.clip(jax.random.uniform(own_keys[7], (2 * STATE,), jnp.float32, -0.5, 0.5), -0.5, 0.5).astype(jnp.bfloat16),
        "dt_bias": draw_dt_bias(jax.random.fold_in(jax.random.fold_in(arg_keys[12], part), 71), part),
        "a_log": draw_a_log(jax.random.fold_in(jax.random.fold_in(arg_keys[12], part), 71), part),
        "d_skip": jnp.clip(0.5 + 1.5 * jax.random.uniform(own_keys[10], (HEADS,), jnp.float32) ** level_of(own_keys[10], (HEADS,), ((0, 2),), -0.2, 0.2), 0.5, 2.0),
        "norm_gain": jnp.clip(1.0 + 0.1 * jax.random.normal(own_keys[11], (DI,), jnp.float32), 0.5, 1.5),
    }


norm_eps = 1e-05

def causal_conv(raw_rows, conv_weight, conv_bias):
    row_count = raw_rows.shape[0]
    padded = jnp.pad(raw_rows, ((CONV - 1, 0), (0, 0))).astype(jnp.float32)
    summed = jnp.zeros(raw_rows.shape, jnp.float32) + conv_bias.astype(jnp.float32)
    for tap_index in range(CONV):
        summed = summed + conv_weight[tap_index].astype(jnp.float32) * padded[tap_index:tap_index + row_count]
    return jax.nn.silu(summed).astype(jnp.bfloat16)

def group_step(state_in, group_data):
    x_group, b_group, c_group, step_group, rate_group = group_data
    log_decay = jnp.cumsum(rate_group, axis=0)
    intersection = jnp.dot(c_group, b_group.T, preferred_element_type=jnp.float32)
    lower_mask = jnp.arange(GROUP)[:, None] >= jnp.arange(GROUP)[None, :]
    head_decay = log_decay.T
    spread = head_decay[:, :, None] - head_decay[:, None, :]
    kernel = jnp.where(lower_mask[None], jnp.exp(jnp.where(lower_mask[None], spread, 0.0)), 0.0)
    mixing = (intersection[None] * kernel * step_group.T[:, None, :]).astype(jnp.bfloat16)
    intra_out = jnp.einsum('hts,shp->thp', mixing.astype(jnp.float32), x_group.astype(jnp.float32))
    carried = jnp.einsum('tn,hpn->thp', c_group.astype(jnp.float32), state_in, precision=lax.Precision.HIGHEST)
    outputs = intra_out + jnp.exp(log_decay)[:, :, None] * carried
    tail_weight = jnp.exp(log_decay[-1][None, :] - log_decay) * step_group
    weighted = (tail_weight[:, :, None] * x_group.astype(jnp.float32)).astype(jnp.bfloat16)
    fresh_state = jnp.einsum('shp,sn->hpn', weighted.astype(jnp.float32), b_group.astype(jnp.float32))
    state_out = jnp.exp(log_decay[-1])[:, None, None] * state_in + fresh_state
    return (state_out, outputs)

def reference(x_raw, bc_raw, gate_in, step_raw, conv_x_weight, conv_x_bias, conv_bc_weight, conv_bc_bias, dt_bias, a_log, d_skip, norm_gain):
    groups = LENGTH // GROUP

    def one_sequence(sequence_data):
        x_rows, bc_rows, gate_rows, step_rows = sequence_data
        x_conv = causal_conv(x_rows, conv_x_weight, conv_x_bias)
        bc_conv = causal_conv(bc_rows, conv_bc_weight, conv_bc_bias)
        step_size = jax.nn.softplus(step_rows + dt_bias)
        log_rate = -jnp.exp(a_log) * step_size
        x_heads = x_conv.reshape(groups, GROUP, HEADS, HEADDIM)
        b_rows = bc_conv[:, :STATE].reshape(groups, GROUP, STATE)
        c_rows = bc_conv[:, STATE:].reshape(groups, GROUP, STATE)
        zero_state = jnp.zeros((HEADS, HEADDIM, STATE), jnp.float32)
        last_state, outputs = lax.scan(group_step, zero_state, (x_heads, b_rows, c_rows, step_size.reshape(groups, GROUP, HEADS), log_rate.reshape(groups, GROUP, HEADS)))
        mixed_rows = outputs.reshape(LENGTH, HEADS, HEADDIM) + d_skip[None, :, None] * x_conv.reshape(LENGTH, HEADS, HEADDIM).astype(jnp.float32)
        gated_rows = mixed_rows.reshape(LENGTH, DI) * jax.nn.silu(gate_rows.astype(jnp.float32))
        mean_square = lax.optimization_barrier(jnp.sum(gated_rows * gated_rows, axis=1, keepdims=True)) / DI
        return (gated_rows * lax.rsqrt(mean_square + norm_eps) * norm_gain).astype(jnp.bfloat16)
    return lax.map(one_sequence, (x_raw, bc_raw, gate_in, step_raw))
```

```python
import functools

import jax
import jax.numpy as jnp
from jax import lax
from jax.experimental import pallas as pl
from jax.experimental.pallas import tpu as pltpu
from jax.sharding import PartitionSpec as P

HEADDIM = 64
STATE = 128
GROUP = 256
CONV = 4
LANE = 128
HALO = 16

norm_eps = 1e-05
F32 = jnp.float32
BF16 = jnp.bfloat16
MESH = pl.DeviceIdType.MESH


def silu(v):
    half = 0.5 * v
    return half * jnp.tanh(half) + half


def pad_lanes(v):
    rows, cols = v.shape
    return jnp.concatenate((v, jnp.zeros((rows, LANE - cols), v.dtype)), axis=1)


def split_pair(v):
    hi = v.astype(BF16).astype(F32)
    lo = v - hi
    lane = lax.broadcasted_iota(jnp.int32, v.shape, 1)
    return jnp.where(lane < 64, hi, pltpu.roll(lo, 64, 1)).astype(BF16)


def mm(a, b):
    return jnp.dot(a, b, preferred_element_type=F32)


def kernel(
    n_seq,
    n_head,
    x_hbm,
    bc_hbm,
    gate_hbm,
    step_hbm,
    wx_ref,
    bx_ref,
    wbc_ref,
    bbc_ref,
    dt_ref,
    alog_ref,
    dskip_ref,
    gain_ref,
    out_hbm,
    xin,
    bcin,
    gate,
    stepin,
    xc,
    bcc,
    bt,
    ld,
    step,
    ldt,
    stept,
    expand,
    wtd,
    fresh,
    gd,
    state,
    state2,
    decay,
    dsk,
    inter,
    y,
    outv,
    tx,
    rx,
    ss_tx,
    ss_rx,
    in_sem,
    out_sem,
    halo_send,
    halo_recv,
    tx_sem,
    rx_sem,
    ss_send,
    ss_recv,
):
    length, feat = xc.shape
    heads = feat // HEADDIM
    groups = length // GROUP
    tiles = feat // LANE
    n_chunk, _, chunk_w = tx.shape
    di = feat * n_head
    me = lax.axis_index("seq")
    me_head = lax.axis_index("head")
    first = me == 0
    last = me == n_seq - 1

    def rows(b):
        return pl.ds(pl.multiple_of(b * GROUP, GROUP), GROUP)

    def rows_in(b):
        return pl.ds(pl.multiple_of(b * GROUP + HALO, HALO), GROUP)

    step_copy = pltpu.make_async_copy(step_hbm.at[0], stepin, in_sem.at[0])
    bc_copy = pltpu.make_async_copy(bc_hbm.at[0], bcin.at[pl.ds(HALO, length)], in_sem.at[1])

    def x_copy(b):
        return pltpu.make_async_copy(x_hbm.at[0, rows(b)], xin.at[rows_in(b)], in_sem.at[2 + b])

    gate_copy = pltpu.make_async_copy(gate_hbm.at[0], gate, in_sem.at[2 + groups])
    step_copy.start()
    bc_copy.start()
    for b in range(groups):
        x_copy(b).start()
    gate_copy.start()

    barrier = pltpu.get_barrier_semaphore()

    @pl.when(jnp.logical_not(first))
    def _():
        pl.semaphore_signal(barrier, inc=1, device_id={"seq": me - 1}, device_id_type=MESH)

    @pl.when(jnp.logical_not(last))
    def _():
        pl.semaphore_signal(barrier, inc=1, device_id={"seq": me + 1}, device_id_type=MESH)

    def mate(r):
        return lax.rem(me_head + r, n_head)

    for r in range(1, n_head):
        pl.semaphore_signal(barrier, inc=1, device_id={"head": mate(r)}, device_id_type=MESH)

    k_of = lax.rem(lax.broadcasted_iota(jnp.int32, (LANE, feat), 0), 64)
    h_of = lax.broadcasted_iota(jnp.int32, (LANE, feat), 1) // HEADDIM
    expand[...] = jnp.where(k_of == h_of, 1.0, 0.0).astype(BF16)
    dsk[...] = mm(
        split_pair(jnp.broadcast_to(pad_lanes(dskip_ref[...]), (8, LANE))), expand[...]
    )

    peers = n_head - 1 + jnp.where(first, 0, 1) + jnp.where(last, 0, 1)
    pl.semaphore_wait(barrier, peers)

    halo_x = pltpu.make_async_remote_copy(
        src_ref=x_hbm.at[0, pl.ds(length - HALO, HALO)],
        dst_ref=xin.at[pl.ds(0, HALO)],
        send_sem=halo_send.at[0],
        recv_sem=halo_recv.at[0],
        device_id={"seq": me + 1},
        device_id_type=MESH,
    )
    halo_bc = pltpu.make_async_remote_copy(
        src_ref=bc_hbm.at[0, pl.ds(length - HALO, HALO)],
        dst_ref=bcin.at[pl.ds(0, HALO)],
        send_sem=halo_send.at[1],
        recv_sem=halo_recv.at[1],
        device_id={"seq": me + 1},
        device_id_type=MESH,
    )

    @pl.when(jnp.logical_not(last))
    def _():
        halo_x.start()
        halo_bc.start()

    @pl.when(first)
    def _():
        xin[0:HALO, :] = jnp.zeros((HALO, feat), BF16)
        bcin[0:HALO, :] = jnp.zeros((HALO, 2 * STATE), BF16)
        rx[...] = jnp.zeros(rx.shape, BF16)

    step_copy.wait()
    dt_row = dt_ref[...]
    rate_row = -jnp.exp(alog_ref[...])
    tri = (
        lax.broadcasted_iota(jnp.int32, (GROUP, GROUP), 0)
        >= lax.broadcasted_iota(jnp.int32, (GROUP, GROUP), 1)
    )
    tri_ones = jnp.where(tri, 1.0, 0.0).astype(BF16)

    def decay_body(b, carry):
        v = stepin[rows(b), :] + dt_row
        size = jnp.maximum(v, 0.0) + jnp.log1p(jnp.exp(-jnp.abs(v)))
        rate = pad_lanes(rate_row * size)
        size = pad_lanes(size)
        hi = rate.astype(BF16)
        rest = rate - hi.astype(F32)
        mid = rest.astype(BF16)
        low = (rest - mid.astype(F32)).astype(BF16)
        total = mm(tri_ones, hi) + mm(tri_ones, mid) + mm(tri_ones, low)
        ld[rows(b), :] = total
        step[rows(b), :] = size
        ldt[b] = total.T[0 : ldt.shape[1]]
        stept[b] = size.T[0 : ldt.shape[1]]
        return carry

    lax.fori_loop(0, groups, decay_body, 0)
    bc_copy.wait()

    def conv(src, start, lo, weight, bias):
        ext = src[pl.ds(pl.multiple_of(start, HALO), GROUP + HALO), lo : lo + LANE].astype(F32)
        w = weight[:, lo : lo + LANE].astype(F32)
        total = bias[0:1, lo : lo + LANE].astype(F32)
        for k in range(CONV):
            off = HALO - CONV + 1 + k
            total = total + w[k : k + 1] * ext[off : off + GROUP]
        return silu(total)

    def fresh_body(i, carry):
        b = lax.rem(i + 1, groups)

        @pl.when(b > 0)
        def _():
            x_copy(b).wait()

        @pl.when(jnp.logical_and(b == 0, jnp.logical_not(first)))
        def _():
            halo_x.wait_recv()
            halo_bc.wait_recv()

        start = b * GROUP
        b_part = conv(bcin, start, 0, wbc_ref, bbc_ref).astype(BF16)
        bcc[rows(b), 0:STATE] = b_part
        bcc[rows(b), STATE : 2 * STATE] = conv(bcin, start, STATE, wbc_ref, bbc_ref).astype(BF16)
        bt[b] = b_part.astype(F32).T.astype(BF16)
        ld_b = ld[rows(b), :]
        end = ld_b[GROUP - 1 : GROUP]
        tail = split_pair(jnp.exp(end - ld_b) * step[rows(b), :])
        gd[b] = mm(split_pair(jnp.broadcast_to(jnp.exp(end), (8, LANE))), expand[...])
        for j in range(tiles):
            lo = j * LANE
            v = conv(xin, start, lo, wx_ref, bx_ref).astype(BF16)
            xc[rows(b), lo : lo + LANE] = v
            weight = mm(tail, expand[:, lo : lo + LANE])
            wtd[:, lo : lo + LANE] = (weight * v.astype(F32)).astype(BF16)
        fresh[b] = mm(bt[b], wtd[...])
        return carry

    x_copy(0).wait()
    lax.fori_loop(0, groups, fresh_body, 0)

    total_state = fresh[0]
    total_decay = gd[0]
    for b in range(1, groups):
        total_state = gd[b, 0:1] * total_state + fresh[b]
        total_decay = total_decay * gd[b]
    state[...] = total_state
    decay[...] = total_decay

    def relay_copy(c):
        return pltpu.make_async_remote_copy(
            src_ref=tx.at[c],
            dst_ref=rx.at[c],
            send_sem=tx_sem.at[c],
            recv_sem=rx_sem.at[c],
            device_id={"seq": me + 1},
            device_id_type=MESH,
        )

    @pl.when(jnp.logical_and(first, jnp.logical_not(last)))
    def _():
        for c in range(n_chunk):
            tx[c] = state[:, c * chunk_w : (c + 1) * chunk_w].astype(BF16)
            relay_copy(c).start()

    def relay(c):
        relay_copy(c).wait_recv()

        @pl.when(jnp.logical_not(last))
        def _():
            cols = pl.ds(pl.multiple_of(c * chunk_w, LANE), chunk_w)
            tx[c] = (decay[0:1, cols] * rx[c].astype(F32) + state[:, cols]).astype(BF16)
            relay_copy(c).start()

    half = GROUP // 2
    low_mask = jnp.where(
        lax.broadcasted_iota(jnp.int32, (1, LANE), 1) < HEADDIM, 1.0, 0.0
    ).astype(BF16)
    high_mask = (1.0 - low_mask.astype(F32)).astype(BF16)
    lag = jnp.minimum(me, 3)
    points = max(1, -(-(n_chunk + 3) // groups))
    marks = [(q + 1) * tiles // points - 1 for q in range(points)]

    def intra_body(b, carry):
        inter[...] = mm(bcc[rows(b), STATE : 2 * STATE], bt[b])
        tri_half = (
            lax.broadcasted_iota(jnp.int32, (half, half), 0)
            >= lax.broadcasted_iota(jnp.int32, (half, half), 1)
        )
        for j in range(tiles):
            lo = j * LANE
            x_pair = xc[rows(b), lo : lo + LANE]
            parts = []
            for e in range(2):
                h = 2 * j + e
                x_own = x_pair * (low_mask if e == 0 else high_mask)
                col = ld[rows(b), h : h + 1]
                row = ldt[b, h : h + 1, :]
                size = stept[b, h : h + 1, :]
                quad = {}
                for ti, si in ((0, 0), (1, 0), (1, 1)):
                    ts, sl = slice(ti * half, (ti + 1) * half), slice(si * half, (si + 1) * half)
                    m = inter[ts, sl] * jnp.exp(col[ts] - row[:, sl]) * size[:, sl]
                    if ti == si:
                        m = jnp.where(tri_half, m, 0.0)
                    quad[ti, si] = m.astype(BF16)
                top = mm(quad[0, 0], x_own[:half])
                bottom = mm(jnp.concatenate((quad[1, 0], quad[1, 1]), axis=1), x_own)
                parts.append((top, bottom))
            skip = dsk[0:1, lo : lo + LANE]
            for ti in range(2):
                at = pl.ds(pl.multiple_of(b * GROUP + ti * half, half), half)
                y[at, lo : lo + LANE] = (
                    parts[0][ti]
                    + parts[1][ti]
                    + skip * x_pair[ti * half : (ti + 1) * half].astype(F32)
                )
            if j in marks:
                c = b * points + marks.index(j) - lag

                @pl.when(
                    jnp.logical_and(
                        jnp.logical_not(first), jnp.logical_and(c >= 0, c < n_chunk)
                    )
                )
                def _():
                    relay(c)

        return carry

    lax.fori_loop(0, groups, intra_body, 0)
    gate_copy.wait()

    for c in range(n_chunk):
        state[:, c * chunk_w : (c + 1) * chunk_w] = rx[c].astype(F32)

    def ss_copy(b, r):
        return pltpu.make_async_remote_copy(
            src_ref=ss_tx.at[b],
            dst_ref=ss_rx.at[b, r],
            send_sem=ss_send.at[b, r],
            recv_sem=ss_recv.at[b, r],
            device_id={"head": mate(r)},
            device_id_type=MESH,
        )

    def gate_body(b, carry):
        now = state[...]
        hi = now.astype(BF16)
        state2[0:STATE, :] = hi
        state2[STATE : 2 * STATE, :] = (now - hi.astype(F32)).astype(BF16)
        state[...] = gd[b, 0:1] * now + fresh[b]
        c_part = bcc[rows(b), STATE : 2 * STATE]
        c_twice = jnp.concatenate((c_part, c_part), axis=1)
        entry = split_pair(jnp.exp(ld[rows(b), :]))
        acc = jnp.zeros((GROUP, LANE), F32)
        for j in range(tiles):
            cols = slice(j * LANE, (j + 1) * LANE)
            carried = mm(c_twice, state2[:, cols])
            scale = mm(entry, expand[:, cols])
            z = (y[rows(b), cols] + scale * carried) * silu(gate[rows(b), cols].astype(F32))
            y[rows(b), cols] = z
            acc = acc + z * z
        sums = jnp.sum(acc.T, axis=0, keepdims=True)
        ss_tx[b] = jnp.broadcast_to(sums, (8, GROUP))
        for r in range(1, n_head):
            ss_copy(b, r).start()
        return carry

    lax.fori_loop(0, groups, gate_body, 0)

    def out_copy(b):
        return pltpu.make_async_copy(outv.at[rows(b)], out_hbm.at[0, rows(b)], out_sem.at[b])

    def norm_body(b, carry):
        sums = ss_tx[b, 0:1]
        for r in range(1, n_head):
            ss_copy(b, r).wait_recv()
            sums = sums + ss_rx[b, r, 0:1]
        scale = lax.rsqrt(sums * (1.0 / di) + norm_eps)
        scale = jnp.broadcast_to(scale, (LANE, GROUP)).T
        for j in range(tiles):
            cols = slice(j * LANE, (j + 1) * LANE)
            outv[rows(b), cols] = (y[rows(b), cols] * scale * gain_ref[0:1, cols]).astype(BF16)
        out_copy(b).start()
        return carry

    lax.fori_loop(0, groups, norm_body, 0)

    for b in range(groups):
        out_copy(b).wait()
        for r in range(1, n_head):
            ss_copy(b, r).wait_send()

    @pl.when(jnp.logical_not(last))
    def _():
        halo_x.wait_send()
        halo_bc.wait_send()
        for c in range(n_chunk):
            relay_copy(c).wait_send()


def on_device(
    x_raw,
    bc_raw,
    gate_in,
    step_raw,
    conv_x_weight,
    conv_x_bias,
    conv_bc_weight,
    conv_bc_bias,
    dt_bias,
    a_log,
    d_skip,
    norm_gain,
):
    length, feat = x_raw.shape[1], x_raw.shape[2]
    heads = dt_bias.shape[0]
    groups = length // GROUP
    tiles = feat // LANE
    n_seq, n_head = lax.axis_size("seq"), lax.axis_size("head")
    n_chunk = tiles // 2 if tiles % 2 == 0 else tiles
    chunk_w = feat // n_chunk
    head_rows = -(-heads // 8) * 8
    anyspec = pl.BlockSpec(memory_space=pl.ANY)
    vspec = pl.BlockSpec(memory_space=pltpu.VMEM)
    V = pltpu.VMEM
    DMA = pltpu.SemaphoreType.DMA
    call = pl.pallas_call(
        functools.partial(kernel, n_seq, n_head),
        out_shape=jax.ShapeDtypeStruct(x_raw.shape, BF16),
        in_specs=[anyspec] * 4 + [vspec] * 8,
        out_specs=anyspec,
        scratch_shapes=[
            V((HALO + length, feat), BF16),
            V((HALO + length, 2 * STATE), BF16),
            V((length, feat), BF16),
            V((length, heads), F32),
            V((length, feat), BF16),
            V((length, 2 * STATE), BF16),
            V((groups, STATE, GROUP), BF16),
            V((length, LANE), F32),
            V((length, LANE), F32),
            V((groups, head_rows, GROUP), F32),
            V((groups, head_rows, GROUP), F32),
            V((LANE, feat), BF16),
            V((GROUP, feat), BF16),
            V((groups, STATE, feat), F32),
            V((groups, 8, feat), F32),
            V((STATE, feat), F32),
            V((2 * STATE, feat), BF16),
            V((8, feat), F32),
            V((8, feat), F32),
            V((GROUP, GROUP), F32),
            V((length, feat), F32),
            V((length, feat), BF16),
            V((n_chunk, STATE, chunk_w), BF16),
            V((n_chunk, STATE, chunk_w), BF16),
            V((groups, 8, GROUP), F32),
            V((groups, n_head, 8, GROUP), F32),
            DMA((3 + groups,)),
            DMA((groups,)),
            DMA((2,)),
            DMA((2,)),
            DMA((n_chunk,)),
            DMA((n_chunk,)),
            DMA((groups, n_head)),
            DMA((groups, n_head)),
        ],
        compiler_params=pltpu.CompilerParams(collective_id=0, has_side_effects=True),
        name="ssd_layer",
    )
    return call(
        x_raw,
        bc_raw,
        gate_in,
        step_raw,
        conv_x_weight,
        conv_x_bias[None],
        conv_bc_weight,
        conv_bc_bias[None],
        dt_bias[None],
        a_log[None],
        d_skip[None],
        norm_gain[None],
    )


def solution(mesh):
    in_specs = (
        P(("member", "rep"), "seq", "head"),
        P(("member", "rep"), "seq", None),
        P(("member", "rep"), "seq", "head"),
        P(("member", "rep"), "seq", "head"),
        P("member", "head"),
        P(("member", "head")),
        P("member", None),
        P("member"),
        P(("member", "head")),
        P(("member", "head")),
        P(("member", "head")),
        P(("member", "head")),
    )
    out_specs = P(("member", "rep"), "seq", "head")
    return jax.shard_map(
        on_device, mesh=mesh, in_specs=in_specs, out_specs=out_specs, check_vma=False
    )
```

```python
import functools

import jax
import jax.numpy as jnp
from jax import lax
from jax.experimental import pallas as pl
from jax.experimental.pallas import tpu as pltpu
from jax.sharding import PartitionSpec as P

HEADDIM = 64
STATE = 128
GROUP = 256
CONV = 4
LANE = 128
HALO = 16
LOG2E = 1.4426950408889634

norm_eps = 1e-05
F32 = jnp.float32
BF16 = jnp.bfloat16
MESH = pl.DeviceIdType.MESH


def silu(v):
    half = 0.5 * v
    return half * jnp.tanh(half) + half


def pad_lanes(v):
    rows, cols = v.shape
    return jnp.concatenate((v, jnp.zeros((rows, LANE - cols), v.dtype)), axis=1)


def split_pair(v):
    hi = v.astype(BF16).astype(F32)
    lo = v - hi
    lane = lax.broadcasted_iota(jnp.int32, v.shape, 1)
    return jnp.where(lane < 64, hi, pltpu.roll(lo, 64, 1)).astype(BF16)


def to_column(row):
    return jnp.broadcast_to(pad_lanes(row), (LANE, LANE)).T[:, 0:1]


def mm(a, b):
    return jnp.dot(a, b, preferred_element_type=F32)


def kernel(
    n_seq,
    n_head,
    x_hbm,
    bc_hbm,
    gate_hbm,
    step_hbm,
    wx_ref,
    bx_ref,
    wbc_ref,
    bbc_ref,
    dt_ref,
    alog_ref,
    dskip_ref,
    y,
    sums_out,
    xin,
    bcin,
    gate,
    stepin,
    xc,
    bcc,
    bt,
    ld,
    step,
    ldt,
    stept,
    ext,
    xtap,
    btap,
    tail,
    acc,
    expand,
    wtd,
    fresh,
    gd,
    state,
    decay,
    dsk,
    inter,
    tx,
    rx,
    ss_tx,
    ss_rx,
    in_sem,
    halo_send,
    halo_recv,
    tx_sem,
    rx_sem,
    ss_send,
    ss_recv,
):
    length, feat = xc.shape
    heads = feat // HEADDIM
    groups = length // GROUP
    tiles = feat // LANE
    n_chunk, _, chunk_w = tx.shape
    di = feat * n_head
    me = lax.axis_index("seq")
    me_head = lax.axis_index("head")
    first = me == 0
    last = me == n_seq - 1

    def rows(b):
        return pl.ds(pl.multiple_of(b * GROUP, GROUP), GROUP)

    def rows_in(b):
        return pl.ds(pl.multiple_of(b * GROUP + HALO, HALO), GROUP)

    step_copy = pltpu.make_async_copy(step_hbm, stepin, in_sem.at[0])
    bc_copy = pltpu.make_async_copy(bc_hbm.at[0], bcin.at[pl.ds(HALO, length)], in_sem.at[1])

    def x_copy(b):
        return pltpu.make_async_copy(x_hbm.at[0, rows(b)], xin.at[rows_in(b)], in_sem.at[2 + b])

    gate_copy = pltpu.make_async_copy(gate_hbm.at[0], gate, in_sem.at[2 + groups])
    step_copy.start()
    bc_copy.start()
    for b in range(groups):
        x_copy(b).start()
    gate_copy.start()

    barrier = pltpu.get_barrier_semaphore()

    @pl.when(jnp.logical_not(first))
    def _():
        pl.semaphore_signal(barrier, inc=1, device_id={"seq": me - 1}, device_id_type=MESH)

    @pl.when(jnp.logical_not(last))
    def _():
        pl.semaphore_signal(barrier, inc=1, device_id={"seq": me + 1}, device_id_type=MESH)

    def mate(r):
        return lax.rem(me_head + r, n_head)

    for r in range(1, n_head):
        pl.semaphore_signal(barrier, inc=1, device_id={"head": mate(r)}, device_id_type=MESH)

    k_of = lax.rem(lax.broadcasted_iota(jnp.int32, (LANE, feat), 0), 64)
    h_of = lax.broadcasted_iota(jnp.int32, (LANE, feat), 1) // HEADDIM
    expand[...] = jnp.where(k_of == h_of, 1.0, 0.0).astype(BF16)
    dsk[...] = mm(
        split_pair(jnp.broadcast_to(pad_lanes(dskip_ref[...]), (8, LANE))), expand[...]
    )

    peers = n_head - 1 + jnp.where(first, 0, 1) + jnp.where(last, 0, 1)
    pl.semaphore_wait(barrier, peers)

    halo_x = pltpu.make_async_remote_copy(
        src_ref=x_hbm.at[0, pl.ds(length - HALO, HALO)],
        dst_ref=xin.at[pl.ds(0, HALO)],
        send_sem=halo_send.at[0],
        recv_sem=halo_recv.at[0],
        device_id={"seq": me + 1},
        device_id_type=MESH,
    )
    halo_bc = pltpu.make_async_remote_copy(
        src_ref=bc_hbm.at[0, pl.ds(length - HALO, HALO)],
        dst_ref=bcin.at[pl.ds(0, HALO)],
        send_sem=halo_send.at[1],
        recv_sem=halo_recv.at[1],
        device_id={"seq": me + 1},
        device_id_type=MESH,
    )

    @pl.when(jnp.logical_not(last))
    def _():
        halo_x.start()
        halo_bc.start()

    @pl.when(first)
    def _():
        xin[0:HALO, :] = jnp.zeros((HALO, feat), BF16)
        bcin[0:HALO, :] = jnp.zeros((HALO, 2 * STATE), BF16)
        rx[...] = jnp.zeros(rx.shape, BF16)

    step_copy.wait()
    dt_col = to_column(dt_ref[...])
    rate_col = to_column(-LOG2E * jnp.exp(alog_ref[...]))
    upto = (
        lax.broadcasted_iota(jnp.int32, (GROUP, GROUP), 0)
        <= lax.broadcasted_iota(jnp.int32, (GROUP, GROUP), 1)
    )
    upto_ones = jnp.where(upto, 1.0, 0.0).astype(BF16)
    ldt[...] = jnp.zeros(ldt.shape, F32)
    stept[...] = jnp.zeros(stept.shape, F32)

    def decay_body(b, carry):
        v = stepin[:, :, rows(b)].reshape(heads, GROUP) + dt_col[:heads]
        size = jnp.maximum(v, 0.0) + jnp.log1p(jnp.exp(-jnp.abs(v)))
        rate = rate_col[:heads] * size
        hi = rate.astype(BF16)
        rest = rate - hi.astype(F32)
        mid = rest.astype(BF16)
        low = (rest - mid.astype(F32)).astype(BF16)
        total = mm(hi, upto_ones) + mm(mid, upto_ones) + mm(low, upto_ones)
        ldt[b, 0:heads, :] = total
        stept[b, 0:heads, :] = size
        ld[rows(b), :] = ldt[b].T
        step[rows(b), :] = stept[b].T
        return carry

    lax.fori_loop(0, groups, decay_body, 0)
    bc_copy.wait()

    def conv(slot, src, start, cols, taps, at):
        ext[slot] = src[pl.ds(pl.multiple_of(start, HALO), GROUP + HALO), cols].astype(F32)
        total = taps[CONV : CONV + 1, at]
        for k in range(CONV):
            total = total + taps[k : k + 1, at] * ext[slot, pl.ds(HALO - CONV + 1 + k, GROUP), :]
        return silu(total)

    xtap[0:CONV, :] = wx_ref[...].astype(F32)
    xtap[CONV : CONV + 1, :] = bx_ref[...].astype(F32)[None]
    btap[0:CONV, :] = wbc_ref[...].astype(F32)
    btap[CONV : CONV + 1, :] = bbc_ref[...].astype(F32)[None]

    def bc_body(i, carry):
        b = lax.rem(i + 1, groups)

        @pl.when(jnp.logical_and(b == 0, jnp.logical_not(first)))
        def _():
            halo_bc.wait_recv()

        start = b * GROUP
        lanes_b, lanes_c = slice(0, STATE), slice(STATE, 2 * STATE)
        b_part = conv(0, bcin, start, lanes_b, btap, lanes_b).astype(BF16)
        bcc[rows(b), 0:STATE] = b_part
        bcc[rows(b), STATE : 2 * STATE] = conv(1, bcin, start, lanes_c, btap, lanes_c).astype(BF16)
        bt[b] = b_part.astype(F32).T.astype(BF16)
        ld_b = ld[rows(b), :]
        end = ld_b[GROUP - 1 : GROUP]
        tail[rows(b), :] = split_pair(jnp.exp2(end - ld_b) * step[rows(b), :])
        gd[b] = mm(split_pair(jnp.broadcast_to(jnp.exp2(end), (8, LANE))), expand[...])
        return carry

    lax.fori_loop(0, groups, bc_body, 0)

    def relay_copy(c):
        return pltpu.make_async_remote_copy(
            src_ref=tx.at[c],
            dst_ref=rx.at[c],
            send_sem=tx_sem.at[c],
            recv_sem=rx_sem.at[c],
            device_id={"seq": me + 1},
            device_id_type=MESH,
        )

    x_copy(0).wait()
    per = chunk_w // LANE

    def fresh_body(i, carry):
        c = i // groups
        b = lax.rem(lax.rem(i, groups) + 1, groups)

        @pl.when(jnp.logical_and(c == 0, b > 0))
        def _():
            x_copy(b).wait()

        @pl.when(jnp.logical_and(jnp.logical_and(c == 0, b == 0), jnp.logical_not(first)))
        def _():
            halo_x.wait_recv()

        wide = pl.ds(pl.multiple_of(c * chunk_w, chunk_w), chunk_w)
        for j in range(per):
            cols = pl.ds(pl.multiple_of(c * chunk_w + j * LANE, LANE), LANE)
            v = conv(j, xin, b * GROUP, cols, xtap, cols).astype(BF16)
            xc[rows(b), cols] = v
            weight = mm(tail[rows(b), :], expand[:, cols])
            wtd[:, j * LANE : (j + 1) * LANE] = (weight * v.astype(F32)).astype(BF16)
        fresh[b, :, wide] = mm(bt[b], wtd[...])

        @pl.when(b == 0)
        def _():
            total_state = fresh[0, :, wide]
            total_decay = gd[0, :, wide]
            for g in range(1, groups):
                total_state = gd[g, 0:1, wide] * total_state + fresh[g, :, wide]
                total_decay = total_decay * gd[g, :, wide]
            state[:, wide] = total_state
            decay[:, wide] = total_decay

            @pl.when(jnp.logical_and(first, jnp.logical_not(last)))
            def _():
                tx[c] = total_state.astype(BF16)
                relay_copy(c).start()

        return carry

    lax.fori_loop(0, groups * n_chunk, fresh_body, 0)

    def relay(c):
        relay_copy(c).wait_recv()

        @pl.when(jnp.logical_not(last))
        def _():
            cols = pl.ds(pl.multiple_of(c * chunk_w, chunk_w), chunk_w)
            tx[c] = (decay[0:1, cols] * rx[c].astype(F32) + state[:, cols]).astype(BF16)
            relay_copy(c).start()

    points = 2
    events = points * groups

    def relay_event(c):
        near = min(max(2 * c - 3, 0), events - 1)
        second = events - 3 + 2 * c if c < 2 else events + min(c - 1, n_chunk - 3)
        return jnp.where(me == 1, near, jnp.where(me == 2, max(second, 0), events + c))

    def relay_at(e):
        for c in range(n_chunk):

            @pl.when(jnp.logical_and(jnp.logical_not(first), relay_event(c) == e))
            def _():
                relay(c)

    half = GROUP // 2
    low_mask = jnp.where(
        lax.broadcasted_iota(jnp.int32, (1, LANE), 1) < HEADDIM, 1.0, 0.0
    ).astype(BF16)
    high_mask = (1.0 - low_mask.astype(F32)).astype(BF16)
    marks = [(q + 1) * tiles // points - 1 for q in range(points)]

    def intra_body(b, carry):
        inter[...] = mm(bcc[rows(b), STATE : 2 * STATE], bt[b])
        tri_half = (
            lax.broadcasted_iota(jnp.int32, (half, half), 0)
            >= lax.broadcasted_iota(jnp.int32, (half, half), 1)
        )
        for j in range(tiles):
            lo = j * LANE
            x_pair = xc[rows(b), lo : lo + LANE]
            parts = []
            for e in range(2):
                h = 2 * j + e
                x_own = x_pair * (low_mask if e == 0 else high_mask)
                col = ld[rows(b), h : h + 1]
                row = ldt[b, h : h + 1, :]
                size = stept[b, h : h + 1, :]
                quad = {}
                for ti, si in ((0, 0), (1, 0), (1, 1)):
                    ts, sl = slice(ti * half, (ti + 1) * half), slice(si * half, (si + 1) * half)
                    m = inter[ts, sl] * jnp.exp2(col[ts] - row[:, sl]) * size[:, sl]
                    if ti == si:
                        m = jnp.where(tri_half, m, 0.0)
                    quad[ti, si] = m.astype(BF16)
                top = mm(quad[0, 0], x_own[:half])
                bottom = mm(jnp.concatenate((quad[1, 0], quad[1, 1]), axis=1), x_own)
                parts.append((top, bottom))
            skip = dsk[0:1, lo : lo + LANE]
            for ti in range(2):
                at = pl.ds(pl.multiple_of(b * GROUP + ti * half, half), half)
                y[at, lo : lo + LANE] = (
                    parts[0][ti]
                    + parts[1][ti]
                    + skip * x_pair[ti * half : (ti + 1) * half].astype(F32)
                )
            if j in marks:
                relay_at(b * points + marks.index(j))

        return carry

    lax.fori_loop(0, groups, intra_body, 0)
    gate_copy.wait()

    def ss_copy(r):
        return pltpu.make_async_remote_copy(
            src_ref=ss_tx,
            dst_ref=ss_rx.at[r],
            send_sem=ss_send.at[r],
            recv_sem=ss_recv.at[r],
            device_id={"head": mate(r)},
            device_id_type=MESH,
        )

    acc[...] = jnp.zeros(acc.shape, F32)

    def entry_body(b, carry):
        tail[rows(b), :] = split_pair(jnp.exp2(ld[rows(b), :]))
        return carry

    lax.fori_loop(0, groups, entry_body, 0)

    def gate_body(c, carry):
        wide = pl.ds(pl.multiple_of(c * chunk_w, chunk_w), chunk_w)
        relay_at(events + c)
        now = rx[c].astype(F32)
        for b in range(groups):
            at = slice(b * GROUP, (b + 1) * GROUP)
            hi = now.astype(BF16)
            both = jnp.concatenate((hi, (now - hi.astype(F32)).astype(BF16)), axis=0)
            if b < groups - 1:
                now = gd[b, 0:1, wide] * now + fresh[b, :, wide]
            c_part = bcc[at, STATE : 2 * STATE]
            carried = mm(jnp.concatenate((c_part, c_part), axis=1), both)
            scale = mm(tail[at, :], expand[:, wide])
            squares = acc[at, :]
            for j in range(per):
                part = slice(j * LANE, (j + 1) * LANE)
                cols = pl.ds(pl.multiple_of(c * chunk_w + j * LANE, LANE), LANE)
                z = y[at, cols] + scale[:, part] * carried[:, part]
                z = z * silu(gate[at, cols].astype(F32))
                y[at, cols] = z
                squares = squares + z * z
            acc[at, :] = squares
        return carry

    lax.fori_loop(0, n_chunk, gate_body, 0)

    for b in range(groups):
        sums = jnp.sum(acc[b * GROUP : (b + 1) * GROUP, :].T, axis=0, keepdims=True)
        ss_tx[b] = jnp.broadcast_to(sums, (8, GROUP))
    for r in range(1, n_head):
        ss_copy(r).start()
    for r in range(1, n_head):
        ss_copy(r).wait_recv()
    for b in range(groups):
        sums = ss_tx[b]
        for r in range(1, n_head):
            sums = sums + ss_rx[r, b]
        sums_out[b] = sums
    for r in range(1, n_head):
        ss_copy(r).wait_send()

    @pl.when(jnp.logical_not(last))
    def _():
        halo_x.wait_send()
        halo_bc.wait_send()
        for c in range(n_chunk):
            relay_copy(c).wait_send()


def norm_kernel(di, y, sums, gain_ref, out):
    feat = out.shape[2]
    scale = lax.rsqrt(sums[0, 0:1] * (1.0 / di) + norm_eps)
    scale = jnp.broadcast_to(scale, (LANE, GROUP)).T
    at = pl.ds(pl.multiple_of(pl.program_id(0) * GROUP, GROUP), GROUP)
    for j in range(feat // LANE):
        cols = slice(j * LANE, (j + 1) * LANE)
        out[0, :, cols] = (y[at, cols] * scale * gain_ref[cols][None]).astype(BF16)


def on_device(
    x_raw,
    bc_raw,
    gate_in,
    step_raw,
    conv_x_weight,
    conv_x_bias,
    conv_bc_weight,
    conv_bc_bias,
    dt_bias,
    a_log,
    d_skip,
    norm_gain,
):
    length, feat = x_raw.shape[1], x_raw.shape[2]
    heads = dt_bias.shape[0]
    groups = length // GROUP
    tiles = feat // LANE
    n_seq, n_head = lax.axis_size("seq"), lax.axis_size("head")
    n_chunk = tiles // 2 if tiles % 2 == 0 else tiles
    chunk_w = feat // n_chunk
    anyspec = pl.BlockSpec(memory_space=pl.ANY)
    vspec = pl.BlockSpec(memory_space=pltpu.VMEM)
    V = pltpu.VMEM
    DMA = pltpu.SemaphoreType.DMA
    vmem_limit = 67043328 - length * feat * 4 - (128 << 10)
    call = pl.pallas_call(
        functools.partial(kernel, n_seq, n_head),
        out_shape=(V((length, feat), F32), jax.ShapeDtypeStruct((groups, 8, GROUP), F32)),
        in_specs=[anyspec] * 4 + [vspec] * 7,
        out_specs=(vspec, vspec),
        scratch_shapes=[
            V((HALO + length, feat), BF16),
            V((HALO + length, 2 * STATE), BF16),
            V((length, feat), BF16),
            V((heads, 1, length), F32),
            V((length, feat), BF16),
            V((length, 2 * STATE), BF16),
            V((groups, STATE, GROUP), BF16),
            V((length, LANE), F32),
            V((length, LANE), F32),
            V((groups, LANE, GROUP), F32),
            V((groups, LANE, GROUP), F32),
            V((2, GROUP + HALO, LANE), F32),
            V((8, feat), F32),
            V((8, 2 * STATE), F32),
            V((length, LANE), BF16),
            V((length, LANE), F32),
            V((LANE, feat), BF16),
            V((GROUP, chunk_w), BF16),
            V((groups, STATE, feat), F32),
            V((groups, 8, feat), F32),
            V((STATE, feat), F32),
            V((8, feat), F32),
            V((8, feat), F32),
            V((GROUP, GROUP), F32),
            V((n_chunk, STATE, chunk_w), BF16),
            V((n_chunk, STATE, chunk_w), BF16),
            V((groups, 8, GROUP), F32),
            V((n_head, groups, 8, GROUP), F32),
            DMA((3 + groups,)),
            DMA((2,)),
            DMA((2,)),
            DMA((n_chunk,)),
            DMA((n_chunk,)),
            DMA((n_head,)),
            DMA((n_head,)),
        ],
        compiler_params=pltpu.CompilerParams(
            collective_id=0, has_side_effects=True, vmem_limit_bytes=vmem_limit
        ),
        name="ssd_layer",
    )
    gated, sums = call(
        x_raw,
        bc_raw,
        gate_in,
        jnp.transpose(step_raw, (2, 0, 1)),
        conv_x_weight,
        conv_x_bias,
        conv_bc_weight,
        conv_bc_bias,
        dt_bias[None],
        a_log[None],
        d_skip[None],
    )
    return pl.pallas_call(
        functools.partial(norm_kernel, feat * n_head),
        grid=(groups,),
        out_shape=jax.ShapeDtypeStruct(x_raw.shape, BF16),
        in_specs=[vspec, pl.BlockSpec((1, 8, GROUP), lambda i: (i, 0, 0)), vspec],
        out_specs=pl.BlockSpec((1, GROUP, feat), lambda i: (0, i, 0)),
        compiler_params=pltpu.CompilerParams(vmem_limit_bytes=16 << 20),
        name="norm",
    )(gated, sums, norm_gain)


def solution(mesh):
    in_specs = (
        P(("member", "rep"), "seq", "head"),
        P(("member", "rep"), "seq", None),
        P(("member", "rep"), "seq", "head"),
        P(("member", "rep"), "seq", "head"),
        P("member", "head"),
        P(("member", "head")),
        P("member", None),
        P("member"),
        P(("member", "head")),
        P(("member", "head")),
        P(("member", "head")),
        P(("member", "head")),
    )
    out_specs = P(("member", "rep"), "seq", "head")
    return jax.shard_map(
        on_device, mesh=mesh, in_specs=in_specs, out_specs=out_specs, check_vma=False
    )
```
